16 devices in a mesh: col: 2 (over z), row: 8 (over y, x, core).
Axes of the slice: x: 2, y: 2, z: 2, core: 2. Of those that a mesh axis runs over, the one named last changes fastest.
Arguments:
- t_amp: float32 [576, 10816], P('row', 'col')
- d_denom: float32 [576, 10816], P('row', 'col')
- v_oovv: bfloat16 [576, 10816], P('row', 'col')
- v_vvvv: bfloat16 [10816, 10816], P('row', 'col')
- v_oooo: bfloat16 [576, 576], replicated
- w_ovov: bfloat16 [2496, 2496], P(None, 'col')
Outputs:
- output: float32 [2496, 2496], P('row', 'col')
All inputs are finite; a program needn't handle non-finite values.
Results may differ from the reference program's by a relative error of at most 0.001.
Values are sent between devices in bfloat16 or wider.
A program may use at most 1 GiB of HBM per device.

```python
import math
import jax
import jax.numpy as jnp
from jax import lax

O = 24
V = 104


def pair_layout(entry_mat):
    entry_four = entry_mat.reshape(O, O, V, V).transpose(0, 2, 1, 3)
    return entry_four.reshape(O * V, O * V)


def setup_inputs(seed: int = 0) -> dict:
    key_list = jax.random.split(jax.random.key(seed), 6)
    amp_scale = 1.5 / math.sqrt(O * V)
    ladder_scale = math.sqrt(O / V)
    hole_scale = math.sqrt(V / O) / 1.5
    t_amp = amp_scale * jax.random.normal(key_list[0], (O * O, V * V), jnp.float32)
    d_denom = -(1.0 + 2.0 * jax.random.uniform(key_list[1], (O * O, V * V), jnp.float32))
    v_oovv = jax.random.normal(key_list[2], (O * O, V * V), jnp.float32).astype(jnp.bfloat16)

    def vvvv_rows(row_block):
        sub_key = jax.random.fold_in(key_list[3], row_block)
        rows_f32 = ladder_scale * jax.random.normal(sub_key, (V, V * V), jnp.float32)
        return rows_f32.astype(jnp.bfloat16)

    v_vvvv = lax.map(vvvv_rows, jnp.arange(V)).reshape(V * V, V * V)
    v_oooo = (hole_scale * jax.random.normal(key_list[4], (O * O, O * O), jnp.float32)).astype(jnp.bfloat16)
    w_ovov = (jax.random.normal(key_list[5], (O * V, O * V), jnp.float32) / 1.5).astype(jnp.bfloat16)
    return {"t_amp": t_amp, "d_denom": d_denom, "v_oovv": v_oovv, "v_vvvv": v_vvvv, "v_oooo": v_oooo, "w_ovov": w_ovov}


def reference(t_amp, d_denom, v_oovv, v_vvvv, v_oooo, w_ovov):
    t_bf = t_amp.astype(jnp.bfloat16)
    r_ladder = jnp.dot(t_bf, v_vvvv, preferred_element_type=jnp.float32)
    x_inter = jnp.dot(v_oovv, t_bf.T, preferred_element_type=jnp.float32)
    w_hole = (v_oooo.astype(jnp.float32) + 0.5 * x_inter).astype(jnp.bfloat16)
    r_hole = jnp.dot(w_hole.T, t_bf, preferred_element_type=jnp.float32)
    entry_sum = v_oovv.astype(jnp.float32) + r_ladder + r_hole
    t_mixed = pair_layout(t_bf)
    r_mixed = jnp.dot(t_mixed, w_ovov, preferred_element_type=jnp.float32)
    return (pair_layout(entry_sum) + r_mixed + r_mixed.T) / pair_layout(d_denom)
```

```python
import functools
import math
import jax
import jax.numpy as jnp
from jax import lax
from jax.experimental import pallas as pl
from jax.experimental.pallas import tpu as pltpu
from jax.sharding import PartitionSpec as P

MESH = pl.DeviceIdType.MESH
CHUNK = 512
HALF = CHUNK // 2


def blk(dk, dy, dx):
    return dk * 4 + dy * 2 + dx


def coords():
    r = lax.axis_index("row")
    c = lax.axis_index("col")
    return r, c, r // 4, (r // 2) % 2, r % 2


def neighbours():
    r, c, y, x, k = coords()
    return {
        "k": {"row": r + 1 - 2 * k},
        "x": {"row": r + 2 * (1 - 2 * x)},
        "y": {"row": r + 4 * (1 - 2 * y)},
        "z": {"col": 1 - c},
    }


def enter(near, extra=()):
    sem = pltpu.get_barrier_semaphore()
    peers = list(near.values()) + list(extra)
    for dev in peers:
        pl.semaphore_signal(sem, inc=1, device_id=dev, device_id_type=MESH)
    pl.semaphore_wait(sem, len(peers))


def rcopy(src, dst, ssem, rsem, dev):
    return pltpu.make_async_remote_copy(
        src_ref=src, dst_ref=dst, send_sem=ssem, recv_sem=rsem, device_id=dev, device_id_type=MESH
    )


def gather_body(p_ref, g_ref, zp_ref, tl_ref, loc_sem, gs, gr, zs, zr, ls, lr):
    r, c, y, x, k = coords()
    near = neighbours()
    diag = {"row": near["x"]["row"] + 1 - 2 * k}
    enter(near, (diag,))
    own = pltpu.make_async_copy(p_ref, g_ref.at[0], loc_sem.at[0])
    own.start()
    bx, by, bd = blk(0, 0, 1), blk(0, 1, 0), blk(0, 1, 1)

    def to_x(q):
        return rcopy(p_ref.at[q], g_ref.at[bx, q], gs.at[bx, q], gr.at[bx, q], near["x"])

    def to_y(q):
        return rcopy(p_ref.at[q], g_ref.at[by, q], gs.at[by, q], gr.at[by, q], near["y"])

    def to_z(q):
        return rcopy(p_ref.at[q], zp_ref.at[q], zs.at[q], zr.at[q], near["z"])

    def to_k(b, q):
        src = p_ref.at[q] if b == 0 else g_ref.at[b, q]
        return rcopy(src, g_ref.at[4 + b, q], gs.at[4 + b, q], gr.at[4 + b, q], near["k"])

    def to_d(q):
        if q < 2:
            return rcopy(g_ref.at[bx, q], g_ref.at[bd, q], gs.at[bd, q], gr.at[bd, q], near["y"])
        return rcopy(g_ref.at[by, q], g_ref.at[bd, q], gs.at[bd, q], gr.at[bd, q], near["x"])

    for s in range(4):
        to_x(s).start()
        to_y((s + 2) % 4).start()
        to_z(s).start()
        to_k(0, s).start()
    for s in range(4):
        to_x(s).wait_recv()
        if s < 2:
            to_d(s).start()
        to_k(bx, s).start()
        q = (s + 2) % 4
        to_y(q).wait_recv()
        if s < 2:
            to_d(q).start()
        to_k(by, q).start()
    for q in range(4):
        to_z(q).wait_recv()
    q_own = 2 * x + k

    def side(dk, dx):
        q = 2 * (x + dx * (1 - 2 * x)) + k + dk * (1 - 2 * k)
        b = blk(dk, 0, dx)
        if dk == 0:
            dev = near["x"]
        else:
            dev = diag if dx else near["k"]
        return rcopy(zp_ref.at[q], tl_ref.at[b], ls.at[b], lr.at[b], dev)

    keep = pltpu.make_async_copy(zp_ref.at[q_own], tl_ref.at[0], loc_sem.at[1])

    @pl.when(y != c)
    def _():
        keep.start()
        for dk, dx in ((0, 1), (1, 1), (1, 0)):
            side(dk, dx).start()

    def up(dk, dx):
        b = blk(dk, 1, dx)
        return rcopy(g_ref.at[b, q_own], tl_ref.at[b], ls.at[b], lr.at[b], near["z"])

    for s in range(4):
        q = (0, 2, 1, 3)[s]
        to_d(q).wait_recv()
        to_k(bd, q).start()
    for q in range(4):
        for b in (by, bx, 0, bd):
            to_k(b, q).wait_recv()

    @pl.when(y == c)
    def _():
        for dk in (0, 1):
            for dx in (0, 1):
                up(dk, dx).start()
        for dk in (0, 1):
            for dx in (0, 1):
                up(dk, dx).wait_send()

    @pl.when(y != c)
    def _():
        keep.wait()
        for dk, dx in ((0, 1), (1, 1), (1, 0)):
            side(dk, dx).wait_send()
            side(dk, dx).wait_recv()
        for dk in (0, 1):
            for dx in (0, 1):
                up(dk, dx).wait_recv()

    own.wait()
    for q in range(4):
        to_x(q).wait_send()
        to_y(q).wait_send()
        to_z(q).wait_send()
        to_d(q).wait_send()
        for b in (0, bx, by, bd):
            to_k(b, q).wait_send()


def gather(p):
    _, rows, cols = p.shape
    dma = pltpu.SemaphoreType.DMA
    any_spec = pl.BlockSpec(memory_space=pl.ANY)
    return pl.pallas_call(
        gather_body,
        name="amp_gather",
        out_shape=(
            jax.ShapeDtypeStruct((8, 4, rows, cols), p.dtype),
            jax.ShapeDtypeStruct((4, rows, cols), p.dtype),
            jax.ShapeDtypeStruct((8, rows, cols), p.dtype),
        ),
        in_specs=[any_spec],
        out_specs=(any_spec, any_spec, any_spec),
        scratch_shapes=[
            dma((2,)), dma((8, 4)), dma((8, 4)), dma((4,)), dma((4,)), dma((8,)), dma((8,)),
        ],
        compiler_params=pltpu.CompilerParams(collective_id=0, has_side_effects=True),
        cost_estimate=pl.CostEstimate(flops=30_000_000_000, bytes_accessed=10_000_000, transcendentals=0),
    )(p)


def ladder_body(n_chunk, lag2, lag3, tl_ref, wt_ref, im_ref, v_ref, t_ref, out_ref,
                sd, ow, rd, sa, sb, ka, kb, ra, rb, s2a, s2b, fa, fb, r2a, r2b,
                ds, dr, as_, ar, bs, br, a2s, a2r, b2s, b2r):
    n = pl.program_id(0)
    r, c, y, x, k = coords()
    near = neighbours()
    rows = t_ref.shape[0]

    @pl.when(n == 0)
    def _():
        enter({key: near[key] for key in ("k", "x", "y")})

    def d2d(m):
        return rcopy(sd.at[m], rd.at[m], ds.at[m], dr.at[m], near["k"])

    def a1(m):
        return rcopy(sa.at[m], ra.at[m], as_.at[m], ar.at[m], near["x"])

    def b1(m):
        return rcopy(sb.at[m], rb.at[m], bs.at[m], br.at[m], near["y"])

    def a2(m):
        return rcopy(s2a.at[m], r2a.at[m], a2s.at[m], a2r.at[m], near["y"])

    def b2(m):
        return rcopy(s2b.at[m], r2b.at[m], b2s.at[m], b2r.at[m], near["x"])

    @pl.when((n >= lag2) & (n < lag2 + n_chunk))
    def _():
        m = n - lag2
        a1(m).wait_recv()
        s2a[m] = ka[m, 1] + ra[m, 1]
        a2(m).start()
        fa[m] = ka[m, 0] + ra[m, 0]
        b1(m).wait_recv()
        s2b[m] = kb[m, 1] + rb[m, 1]
        b2(m).start()
        fb[m] = kb[m, 0] + rb[m, 0]

    @pl.when((n >= 1) & (n < 1 + n_chunk))
    def _():
        m = n - 1
        d2d(m).wait_recv()

        def tot(dy, dx, lo):
            b = dy * 2 + dx
            return ow[m, b, :, lo:lo + HALF] + rd[m, b, :, lo:lo + HALF]

        for dy in (0, 1):
            sa[m, dy] = tot(dy, 1, 0)
        a1(m).start()
        for dx in (0, 1):
            sb[m, dx] = tot(1, dx, HALF)
        b1(m).start()
        for dy in (0, 1):
            ka[m, dy] = tot(dy, 0, 0)
        for dx in (0, 1):
            kb[m, dx] = tot(0, dx, HALF)

    @pl.when(n < n_chunk)
    def _():
        row_id = lax.broadcasted_iota(jnp.int32, (rows, CHUNK), 0)
        seg = rows // 6
        base_row = y * (rows // 2) + 3 * (r % 4)
        for dk in (1, 0):
            half = 4 * rows
            lhs = tl_ref[dk * half:(dk + 1) * half, :]
            part = jnp.dot(lhs, v_ref[...], preferred_element_type=jnp.float32)
            part += jnp.dot(wt_ref[dk * half:(dk + 1) * half, :], t_ref[...], preferred_element_type=jnp.float32)
            for b in range(4):
                acc = part[b * rows:(b + 1) * rows]
                for i in range(3):
                    for e in range(3):
                        im_row = im_ref[dk * 4 + b, 3 * i + e:3 * i + e + 1, :]
                        acc = acc + jnp.where(row_id == base_row + seg * i + e, im_row, 0.0)
                if dk:
                    sd[n, b] = acc
                else:
                    ow[n, b] = acc
            if dk:
                d2d(n).start()

    @pl.when(n >= lag3)
    def _():
        m = n - lag3
        a2(m).wait_recv()
        col = pl.multiple_of(m * CHUNK, CHUNK)
        out_ref[:, pl.ds(col, HALF)] = fa[m] + r2a[m]
        b2(m).wait_recv()
        colb = pl.multiple_of(m * CHUNK + HALF, HALF)
        out_ref[:, pl.ds(colb, HALF)] = fb[m] + r2b[m]

    @pl.when(n == lag3 + n_chunk - 1)
    def _():
        def drain(m, carry):
            for one in (d2d, a1, b1, a2, b2):
                one(m).wait_send()
            return carry

        lax.fori_loop(0, n_chunk, drain, 0)


def ladder(tl, wt, im, v, t):
    rows, n_col = t.shape
    n_chunk = -(-n_col // CHUNK)
    lag2, lag3 = 3, 5
    depth = v.shape[0]
    last = n_chunk - 1
    dma = pltpu.SemaphoreType.DMA
    f32 = jnp.float32
    vm = lambda *s: pltpu.VMEM((n_chunk,) + s, f32)
    return pl.pallas_call(
        functools.partial(ladder_body, n_chunk, lag2, lag3),
        name="ladder_rs",
        grid=(n_chunk + lag3,),
        out_shape=jax.ShapeDtypeStruct((rows, n_chunk * CHUNK), f32),
        in_specs=[
            pl.BlockSpec((8 * rows, depth), lambda n: (0, 0)),
            pl.BlockSpec((8 * rows, rows), lambda n: (0, 0)),
            pl.BlockSpec((8, 9, CHUNK), lambda n: (0, 0, jnp.minimum(n, last))),
            pl.BlockSpec((depth, CHUNK), lambda n: (0, jnp.minimum(n, last))),
            pl.BlockSpec((rows, CHUNK), lambda n: (0, jnp.minimum(n, last))),
        ],
        out_specs=pl.BlockSpec((rows, n_chunk * CHUNK), lambda n: (0, 0)),
        scratch_shapes=[
            vm(4, rows, CHUNK), vm(4, rows, CHUNK), vm(4, rows, CHUNK),
            vm(2, rows, HALF), vm(2, rows, HALF), vm(2, rows, HALF), vm(2, rows, HALF),
            vm(2, rows, HALF), vm(2, rows, HALF),
            vm(rows, HALF), vm(rows, HALF), vm(rows, HALF), vm(rows, HALF), vm(rows, HALF), vm(rows, HALF),
        ] + [dma((n_chunk,))] * 10,
        compiler_params=pltpu.CompilerParams(
            collective_id=1, has_side_effects=True, vmem_limit_bytes=60 * 1024 * 1024,
            dimension_semantics=("arbitrary",),
        ),
        cost_estimate=pl.CostEstimate(flops=60_000_000_000, bytes_accessed=30_000_000, transcendentals=0),
    )(tl, wt, im, v, t)


def relative(a, r, axis):
    shape = a.shape
    a = a.reshape(shape[:axis] + (2, 2, 2) + shape[axis + 1:])
    for bit, ax in ((r // 4, axis), ((r // 2) % 2, axis + 1), (r % 2, axis + 2)):
        a = jnp.where(bit == 1, jnp.flip(a, ax), a)
    perm = list(range(a.ndim))
    perm[axis:axis + 3] = [axis + 2, axis, axis + 1]
    return a.transpose(perm).reshape(shape)


def solution(mesh):
    row_n = mesh.shape["row"]
    col_n = mesh.shape["col"]
    swap_z = [(0, 1), (1, 0)]

    def local_sweep(t_blk, d_blk, voovv_blk, vvvvv_blk, oooo_blk, wr_blk):
        n_occ = math.isqrt(oooo_blk.shape[1])
        n_vir = wr_blk.shape[0] // n_occ
        o_r = n_occ // row_n
        o_c = n_occ // col_n
        v_c = n_vir // col_n
        rows = o_r * n_occ
        n_col = v_c * n_vir
        piece = n_col // 4
        r, c, y, x, k = coords()
        f32 = jnp.float32

        d_rows = d_blk.reshape(o_r, 2, o_c, n_col)
        d_send = lax.dynamic_index_in_dim(d_rows, 1 - c, 1, keepdims=False)
        d_keep = lax.dynamic_index_in_dim(d_rows, c, 1, keepdims=False)
        d_recv = lax.ppermute(d_send, "col", swap_z)

        t_bf = t_blk.astype(jnp.bfloat16)
        p = t_bf.reshape(o_r, 2, o_c, 4, piece).transpose(3, 1, 0, 2, 4).reshape(4, rows, piece)
        g, zp, tl_recv = gather(p)

        tm_own = t_bf.reshape(o_r, n_occ, v_c, n_vir).transpose(0, 2, 1, 3).reshape(o_r * v_c, n_occ * n_vir)
        tm_oth = zp.reshape(4, 2, o_r, o_c, v_c // 4, n_vir).transpose(2, 0, 4, 1, 3, 5)
        tm_oth = tm_oth.reshape(o_r * v_c, n_occ * n_vir)
        r3_own = jnp.dot(tm_own, wr_blk, preferred_element_type=f32)
        r3_oth = jnp.dot(tm_oth, wr_blk, preferred_element_type=f32)

        def order(own, oth, axis):
            lo = jnp.where(c == 0, own, oth)
            hi = jnp.where(c == 0, oth, own)
            return jnp.concatenate([lo, hi], axis=axis)

        r3 = order(r3_own.reshape(o_r, v_c, o_c * n_vir), r3_oth.reshape(o_r, v_c, o_c * n_vir), 1)
        r3_t = r3.reshape(o_r, n_vir, o_c, 2, v_c).transpose(3, 2, 0, 4, 1)
        im_send = lax.dynamic_index_in_dim(r3_t, 1 - c, 0, keepdims=False).reshape(o_c, o_r, n_col)
        im_keep = lax.dynamic_index_in_dim(r3_t, c, 0, keepdims=False).reshape(o_c, o_r, n_col)
        im_recv = lax.ppermute(im_send, "col", swap_z)
        im = order(im_keep, im_recv, 0).reshape(row_n, o_r * o_r, n_col)
        im = relative(im, r, 0)

        x_part = sum(
            lax.dot_general(voovv_blk[:, q * piece:(q + 1) * piece], g[:, q].reshape(row_n * rows, piece),
                            (((1,), (1,)), ((), ())), preferred_element_type=f32)
            for q in range(4)
        )
        x_full = x_part + lax.ppermute(x_part, "col", swap_z)
        oooo = oooo_blk.reshape(rows, row_n, o_r, 2, o_c).transpose(0, 1, 3, 2, 4).reshape(rows, row_n, rows)
        oooo = relative(oooo, r, 1).reshape(rows, row_n * rows)
        w_hole = (oooo.astype(f32) + 0.5 * x_full).astype(jnp.bfloat16)

        q_own = 2 * x + k
        tl = jnp.where(y == c, lax.dynamic_index_in_dim(g, q_own, 1, keepdims=False), tl_recv)
        base = ladder(tl.reshape(row_n * rows, piece), w_hole.T, im, vvvvv_blk, t_bf)
        base = base[:, :n_col].reshape(2, o_r, o_c, n_col)
        vo_rows = voovv_blk.reshape(o_r, 2, o_c, n_col).transpose(1, 0, 2, 3)
        base = base + vo_rows.astype(f32)
        b_recv = lax.ppermute(lax.dynamic_index_in_dim(base, 1 - c, 0, keepdims=False), "col", swap_z)
        b_keep = lax.dynamic_index_in_dim(base, c, 0, keepdims=False)

        def mixed(own, oth):
            both = order(own.reshape(o_r, o_c, v_c, n_vir), oth.reshape(o_r, o_c, v_c, n_vir), 2)
            return both.transpose(0, 2, 1, 3).reshape(o_r * n_vir, o_c * n_vir)

        return (mixed(b_keep, b_recv) + r3.reshape(o_r * n_vir, o_c * n_vir)) / mixed(d_keep, d_recv)

    return jax.shard_map(
        local_sweep,
        mesh=mesh,
        in_specs=(P("row", "col"), P("row", "col"), P("row", "col"), P("row", "col"), P("row", None), P(None, "col")),
        out_specs=P("row", "col"),
        check_vma=False,
    )
```

```python
import functools
import math
import jax
import jax.numpy as jnp
from jax import lax
from jax.experimental import pallas as pl
from jax.experimental.pallas import tpu as pltpu
from jax.sharding import PartitionSpec as P

MESH = pl.DeviceIdType.MESH
CHUNK = 512
HALF = CHUNK // 2


def blk(dk, dy, dx):
    return dk * 4 + dy * 2 + dx


def coords():
    r = lax.axis_index("row")
    c = lax.axis_index("col")
    return r, c, r // 4, (r // 2) % 2, r % 2


def neighbours():
    r, c, y, x, k = coords()
    return {
        "k": {"row": r + 1 - 2 * k},
        "x": {"row": r + 2 * (1 - 2 * x)},
        "y": {"row": r + 4 * (1 - 2 * y)},
        "z": {"col": 1 - c},
    }


def enter(near, extra=()):
    sem = pltpu.get_barrier_semaphore()
    peers = list(near.values()) + list(extra)
    for dev in peers:
        pl.semaphore_signal(sem, inc=1, device_id=dev, device_id_type=MESH)
    pl.semaphore_wait(sem, len(peers))


def rcopy(src, dst, ssem, rsem, dev):
    return pltpu.make_async_remote_copy(
        src_ref=src, dst_ref=dst, send_sem=ssem, recv_sem=rsem, device_id=dev, device_id_type=MESH
    )


def gather_body(p_ref, g_ref, zp_ref, tl_ref, loc_sem, gs, gr, zs, zr, ls, lr):
    r, c, y, x, k = coords()
    near = neighbours()
    diag = {"row": near["x"]["row"] + 1 - 2 * k}
    enter(near, (diag,))
    own = pltpu.make_async_copy(p_ref, g_ref.at[0], loc_sem.at[0])
    own.start()
    bx, by, bd = blk(0, 0, 1), blk(0, 1, 0), blk(0, 1, 1)

    def to_x(q):
        return rcopy(p_ref.at[q], g_ref.at[bx, q], gs.at[bx, q], gr.at[bx, q], near["x"])

    def to_y(q):
        return rcopy(p_ref.at[q], g_ref.at[by, q], gs.at[by, q], gr.at[by, q], near["y"])

    def to_z(q):
        return rcopy(p_ref.at[q], zp_ref.at[q], zs.at[q], zr.at[q], near["z"])

    def to_k(b, q):
        src = p_ref.at[q] if b == 0 else g_ref.at[b, q]
        return rcopy(src, g_ref.at[4 + b, q], gs.at[4 + b, q], gr.at[4 + b, q], near["k"])

    def to_d(q):
        if q < 2:
            return rcopy(g_ref.at[bx, q], g_ref.at[bd, q], gs.at[bd, q], gr.at[bd, q], near["y"])
        return rcopy(g_ref.at[by, q], g_ref.at[bd, q], gs.at[bd, q], gr.at[bd, q], near["x"])

    for s in range(4):
        to_x(s).start()
        to_y((s + 2) % 4).start()
        to_z(s).start()
        to_k(0, s).start()
    for s in range(4):
        to_x(s).wait_recv()
        if s < 2:
            to_d(s).start()
        to_k(bx, s).start()
        q = (s + 2) % 4
        to_y(q).wait_recv()
        if s < 2:
            to_d(q).start()
        to_k(by, q).start()
    for q in range(4):
        to_z(q).wait_recv()
    q_own = 2 * x + k

    def side(dk, dx):
        q = 2 * (x + dx * (1 - 2 * x)) + k + dk * (1 - 2 * k)
        b = blk(dk, 0, dx)
        if dk == 0:
            dev = near["x"]
        else:
            dev = diag if dx else near["k"]
        return rcopy(zp_ref.at[q], tl_ref.at[b], ls.at[b], lr.at[b], dev)

    keep = pltpu.make_async_copy(zp_ref.at[q_own], tl_ref.at[0], loc_sem.at[1])

    @pl.when(y != c)
    def _():
        keep.start()
        for dk, dx in ((0, 1), (1, 1), (1, 0)):
            side(dk, dx).start()

    def up(dk, dx):
        b = blk(dk, 1, dx)
        return rcopy(g_ref.at[b, q_own], tl_ref.at[b], ls.at[b], lr.at[b], near["z"])

    for s in range(4):
        q = (0, 2, 1, 3)[s]
        to_d(q).wait_recv()
        to_k(bd, q).start()
    for q in range(4):
        for b in (by, bx, 0, bd):
            to_k(b, q).wait_recv()

    @pl.when(y == c)
    def _():
        for dk in (0, 1):
            for dx in (0, 1):
                up(dk, dx).start()
        for dk in (0, 1):
            for dx in (0, 1):
                up(dk, dx).wait_send()

    @pl.when(y != c)
    def _():
        keep.wait()
        for dk, dx in ((0, 1), (1, 1), (1, 0)):
            side(dk, dx).wait_send()
            side(dk, dx).wait_recv()
        for dk in (0, 1):
            for dx in (0, 1):
                up(dk, dx).wait_recv()

    own.wait()
    for q in range(4):
        to_x(q).wait_send()
        to_y(q).wait_send()
        to_z(q).wait_send()
        to_d(q).wait_send()
        for b in (0, bx, by, bd):
            to_k(b, q).wait_send()


def gather(p):
    _, rows, cols = p.shape
    dma = pltpu.SemaphoreType.DMA
    any_spec = pl.BlockSpec(memory_space=pl.ANY)
    return pl.pallas_call(
        gather_body,
        name="amp_gather",
        out_shape=(
            jax.ShapeDtypeStruct((8, 4, rows, cols), p.dtype),
            jax.ShapeDtypeStruct((4, rows, cols), p.dtype),
            jax.ShapeDtypeStruct((8, rows, cols), p.dtype),
        ),
        in_specs=[any_spec],
        out_specs=(any_spec, any_spec, any_spec),
        scratch_shapes=[
            dma((2,)), dma((8, 4)), dma((8, 4)), dma((4,)), dma((4,)), dma((8,)), dma((8,)),
        ],
        compiler_params=pltpu.CompilerParams(collective_id=0, has_side_effects=True),
        cost_estimate=pl.CostEstimate(flops=30_000_000_000, bytes_accessed=10_000_000, transcendentals=0),
    )(p)


def ladder_body(n_chunk, lag2, lag3, tl_ref, wt_ref, v_ref, t_ref, vo_ref, im_ref, d_ref, base_ref, brecv_ref, drecv_ref,
                sd, ow, rd, sa, sb, ka, kb, ra, rb, s2a, s2b, fa, fb, r2a, r2b, fin, imv,
                ds, dr, as_, ar, bs, br, a2s, a2r, b2s, b2r, zs, zr, ims, imr, dds, ddr, iml):
    n = pl.program_id(0)
    r, c, y, x, k = coords()
    near = neighbours()
    rows = t_ref.shape[0]
    win = brecv_ref.shape[0]
    dwin = drecv_ref.shape[0] // 3

    def d2d(m):
        return rcopy(sd.at[m], rd.at[m], ds.at[m], dr.at[m], near["k"])

    def a1(m):
        return rcopy(sa.at[m], ra.at[m], as_.at[m], ar.at[m], near["x"])

    def b1(m):
        return rcopy(sb.at[m], rb.at[m], bs.at[m], br.at[m], near["y"])

    def a2(m):
        return rcopy(s2a.at[m], r2a.at[m], a2s.at[m], a2r.at[m], near["y"])

    def b2(m):
        return rcopy(s2b.at[m], r2b.at[m], b2s.at[m], b2r.at[m], near["x"])

    def zb(m):
        off = pl.multiple_of((rows - win) * (1 - c), 8)
        col = pl.multiple_of(m * CHUNK, CHUNK)
        return rcopy(fin.at[m, pl.ds(off, win)], brecv_ref.at[:, pl.ds(col, CHUNK)], zs.at[m], zr.at[m], near["z"])

    def zim(m):
        return rcopy(im_ref.at[1 - c, m], imv.at[c, m], ims.at[m], imr.at[m], near["z"])

    def zim_in(m):
        return rcopy(im_ref.at[1 - c, m], imv.at[1 - c, m], ims.at[m], imr.at[m], near["z"])

    def im_own():
        return pltpu.make_async_copy(im_ref.at[c], imv.at[c], iml.at[0])

    def zd(i):
        off = pl.multiple_of(i * (rows // 3) + 8 * (1 - c), 8)
        return rcopy(d_ref.at[pl.ds(off, dwin)], drecv_ref.at[pl.ds(i * dwin, dwin)], dds.at[i], ddr.at[i], near["z"])

    @pl.when(n == 0)
    def _():
        enter(near)
        im_own().start()
        for m in range(n_chunk):
            zim(m).start()
        for i in range(3):
            zd(i).start()

    @pl.when((n >= lag2) & (n < lag2 + n_chunk))
    def _():
        m = n - lag2
        a1(m).wait_recv()
        s2a[m] = ka[m, 1] + ra[m, 1]
        a2(m).start()
        fa[m] = ka[m, 0] + ra[m, 0]
        b1(m).wait_recv()
        s2b[m] = kb[m, 1] + rb[m, 1]
        b2(m).start()
        fb[m] = kb[m, 0] + rb[m, 0]

    @pl.when((n >= 1) & (n < 1 + n_chunk))
    def _():
        m = n - 1
        d2d(m).wait_recv()

        def tot(dy, dx, lo):
            b = dy * 2 + dx
            return ow[m, b, :, lo:lo + HALF] + rd[m, b, :, lo:lo + HALF]

        for dy in (0, 1):
            sa[m, dy] = tot(dy, 1, 0)
        a1(m).start()
        for dx in (0, 1):
            sb[m, dx] = tot(1, dx, HALF)
        b1(m).start()
        for dy in (0, 1):
            ka[m, dy] = tot(dy, 0, 0)
        for dx in (0, 1):
            kb[m, dx] = tot(0, dx, HALF)

    @pl.when(n == 0)
    def _():
        im_own().wait()

    @pl.when(n < n_chunk)
    def _():
        zim_in(n).wait_recv()
        row_id = lax.broadcasted_iota(jnp.int32, (rows, CHUNK), 0)
        seg = rows // 6
        base_row = y * (rows // 2) + 3 * (r % 4)
        for dk in (1, 0):
            half = 4 * rows
            lhs = tl_ref[dk * half:(dk + 1) * half, :]
            part = jnp.dot(lhs, v_ref[...], preferred_element_type=jnp.float32)
            part += jnp.dot(wt_ref[dk * half:(dk + 1) * half, :], t_ref[...], preferred_element_type=jnp.float32)
            for dy in (0, 1):
                y_b = y + dy * (1 - 2 * y)
                for dx in (0, 1):
                    b = dy * 2 + dx
                    bl = 2 * (x + dx * (1 - 2 * x)) + k + dk * (1 - 2 * k)
                    acc = part[b * rows:(b + 1) * rows]
                    for i in range(3):
                        for e in range(3):
                            im_row = imv[y_b, n, pl.ds(e * seg + 3 * bl + i, 1), :]
                            acc = acc + jnp.where(row_id == base_row + seg * i + e, im_row, 0.0)
                    if dk:
                        sd[n, b] = acc
                    else:
                        ow[n, b] = acc
            if dk:
                d2d(n).start()

    @pl.when(n >= lag3)
    def _():
        m = n - lag3
        a2(m).wait_recv()
        fin[m, :, 0:HALF] = fa[m] + r2a[m] + vo_ref[:, 0:HALF].astype(jnp.float32)
        b2(m).wait_recv()
        fin[m, :, HALF:CHUNK] = fb[m] + r2b[m] + vo_ref[:, HALF:CHUNK].astype(jnp.float32)
        zb(m).start()
        base_ref[:, pl.ds(pl.multiple_of(m * CHUNK, CHUNK), CHUNK)] = fin[m]

    @pl.when(n == lag3 + n_chunk - 1)
    def _():
        def drain(m, carry):
            for one in (d2d, a1, b1, a2, b2, zb, zim):
                one(m).wait_send()
            zb(m).wait_recv()
            return carry

        lax.fori_loop(0, n_chunk, drain, 0)
        for i in range(3):
            zd(i).wait_send()
            zd(i).wait_recv()


def ladder(tl, wt, v, t, vo, im, d):
    rows, n_col = t.shape
    n_chunk = -(-n_col // CHUNK)
    lag2, lag3 = 3, 5
    depth = v.shape[0]
    last = n_chunk - 1
    win = im.shape[2]
    dwin = 16
    wide = n_chunk * CHUNK
    dma = pltpu.SemaphoreType.DMA
    f32 = jnp.float32
    vm = lambda *s: pltpu.VMEM((n_chunk,) + s, f32)
    any_spec = pl.BlockSpec(memory_space=pl.ANY)
    return pl.pallas_call(
        functools.partial(ladder_body, n_chunk, lag2, lag3),
        name="ladder_rs",
        grid=(n_chunk + lag3,),
        out_shape=(
            jax.ShapeDtypeStruct((rows, wide), f32),
            jax.ShapeDtypeStruct((win, wide), f32),
            jax.ShapeDtypeStruct((3 * dwin, n_col), f32),
        ),
        in_specs=[
            pl.BlockSpec((8 * rows, depth), lambda n: (0, 0)),
            pl.BlockSpec((8 * rows, rows), lambda n: (0, 0)),
            pl.BlockSpec((depth, CHUNK), lambda n: (0, jnp.minimum(n, last))),
            pl.BlockSpec((rows, CHUNK), lambda n: (0, jnp.minimum(n, last))),
            pl.BlockSpec((rows, CHUNK), lambda n: (0, jnp.maximum(n - lag3, 0))),
            any_spec,
            any_spec,
        ],
        out_specs=(pl.BlockSpec((rows, wide), lambda n: (0, 0)), any_spec, any_spec),
        scratch_shapes=[
            vm(4, rows, CHUNK), vm(4, rows, CHUNK), vm(4, rows, CHUNK),
            vm(2, rows, HALF), vm(2, rows, HALF), vm(2, rows, HALF), vm(2, rows, HALF),
            vm(2, rows, HALF), vm(2, rows, HALF),
            vm(rows, HALF), vm(rows, HALF), vm(rows, HALF), vm(rows, HALF), vm(rows, HALF), vm(rows, HALF),
            vm(rows, CHUNK), pltpu.VMEM((2, n_chunk, win, CHUNK), f32),
        ] + [dma((n_chunk,))] * 14 + [dma((3,)), dma((3,)), dma((1,))],
        compiler_params=pltpu.CompilerParams(
            collective_id=1, has_side_effects=True, vmem_limit_bytes=60 * 1024 * 1024,
            dimension_semantics=("arbitrary",),
        ),
        cost_estimate=pl.CostEstimate(flops=60_000_000_000, bytes_accessed=30_000_000, transcendentals=0),
    )(tl, wt, v, t, vo, im, d)


def finish_body(n_vir, base_ref, brecv_ref, d_ref, drecv_ref, r3_ref, out_ref, sb, sd):
    c = lax.axis_index("col")
    rows = base_ref.shape[0]
    win = brecv_ref.shape[0]
    dwin = drecv_ref.shape[0] // 3
    o_c = rows // 6
    v_c = n_vir // 2
    off = pl.multiple_of((rows - win) * c, 8)
    for a in range(v_c):
        lanes = slice(a * n_vir, (a + 1) * n_vir)
        sb[c, a * win:(a + 1) * win, 0:n_vir] = base_ref[pl.ds(off, win), lanes]
        sb[1 - c, a * win:(a + 1) * win, 0:n_vir] = brecv_ref[:, lanes]
        for i in range(3):
            at = (a * 3 + i) * dwin
            sd[c, at:at + dwin, 0:n_vir] = d_ref[pl.ds(pl.multiple_of(i * (rows // 3) + 8 * c, 8), dwin), lanes]
            sd[1 - c, at:at + dwin, 0:n_vir] = drecv_ref[i * dwin:(i + 1) * dwin, lanes]
    for h in range(2):
        for i in range(3):
            out_rows = slice(i * n_vir + h * v_c, i * n_vir + (h + 1) * v_c)
            for j in range(o_c):
                cols = slice(j * n_vir, (j + 1) * n_vir)
                num = sb[h, pl.ds(4 * c + i * o_c + j, v_c, stride=win), :]
                den = sd[h, pl.ds(4 * c + i * dwin + j, v_c, stride=3 * dwin), :]
                out_ref[out_rows, cols] = (num[:, 0:n_vir] + r3_ref[out_rows, cols]) / den[:, 0:n_vir]


def finish(base, brecv, d, drecv, r3, n_vir):
    v_c = n_vir // 2
    f32 = jnp.float32
    return pl.pallas_call(
        functools.partial(finish_body, n_vir),
        name="finish",
        out_shape=jax.ShapeDtypeStruct(r3.shape, f32),
        in_specs=[pl.BlockSpec(memory_space=pltpu.VMEM)] * 5,
        out_specs=pl.BlockSpec(memory_space=pltpu.VMEM),
        scratch_shapes=[
            pltpu.VMEM((2, v_c * brecv.shape[0], 128), f32),
            pltpu.VMEM((2, v_c * drecv.shape[0], 128), f32),
        ],
        compiler_params=pltpu.CompilerParams(vmem_limit_bytes=60 * 1024 * 1024),
    )(base, brecv, d, drecv, r3)


def relative(a, r, axis):
    shape = a.shape
    a = a.reshape(shape[:axis] + (2, 2, 2) + shape[axis + 1:])
    for bit, ax in ((r // 4, axis), ((r // 2) % 2, axis + 1), (r % 2, axis + 2)):
        a = jnp.where(bit == 1, jnp.flip(a, ax), a)
    perm = list(range(a.ndim))
    perm[axis:axis + 3] = [axis + 2, axis, axis + 1]
    return a.transpose(perm).reshape(shape)


def solution(mesh):
    row_n = mesh.shape["row"]
    col_n = mesh.shape["col"]
    swap_z = [(0, 1), (1, 0)]

    def local_sweep(t_blk, d_blk, voovv_blk, vvvvv_blk, oooo_blk, wr_blk):
        n_occ = math.isqrt(oooo_blk.shape[1])
        n_vir = wr_blk.shape[0] // n_occ
        o_r = n_occ // row_n
        o_c = n_occ // col_n
        v_c = n_vir // col_n
        rows = o_r * n_occ
        n_col = v_c * n_vir
        piece = n_col // 4
        r, c, y, x, k = coords()
        f32 = jnp.float32

        t_bf = t_blk.astype(jnp.bfloat16)
        t_perm = t_bf.reshape(o_r, 2, o_c, n_col).transpose(1, 0, 2, 3).reshape(rows, n_col)
        p = t_perm.reshape(rows, 4, piece).transpose(1, 0, 2)
        vo_perm = voovv_blk.reshape(o_r, 2, o_c, n_col).transpose(1, 0, 2, 3).reshape(rows, n_col)
        g, zp, tl_recv = gather(p)

        tm_own = t_bf.reshape(o_r, n_occ, v_c, n_vir).transpose(0, 2, 1, 3).reshape(o_r * v_c, n_occ * n_vir)
        tm_oth = zp.reshape(4, 2, o_r, o_c, v_c // 4, n_vir).transpose(2, 0, 4, 1, 3, 5)
        tm_oth = tm_oth.reshape(o_r * v_c, n_occ * n_vir)
        r3_own = jnp.dot(tm_own, wr_blk, preferred_element_type=f32)
        r3_oth = jnp.dot(tm_oth, wr_blk, preferred_element_type=f32)

        def order(own, oth, axis):
            lo = jnp.where(c == 0, own, oth)
            hi = jnp.where(c == 0, oth, own)
            return jnp.concatenate([lo, hi], axis=axis)

        r3 = order(r3_own.reshape(o_r, v_c, o_c * n_vir), r3_oth.reshape(o_r, v_c, o_c * n_vir), 1)
        r3_t = r3.reshape(o_r, n_vir, o_c, 2, v_c).transpose(3, 0, 2, 4, 1).reshape(2, o_r * o_c, n_col)
        wide = -(-n_col // CHUNK) * CHUNK
        im = jnp.pad(r3_t, ((0, 0), (0, 4), (0, wide - n_col)))
        im = im.reshape(2, rows // 2 + 4, wide // CHUNK, CHUNK).transpose(0, 2, 1, 3)

        x_part = sum(
            lax.dot_general(vo_perm[:, q * piece:(q + 1) * piece], g[:, q].reshape(row_n * rows, piece),
                            (((1,), (1,)), ((), ())), preferred_element_type=f32)
            for q in range(4)
        )
        x_full = x_part + lax.ppermute(x_part, "col", swap_z)
        oooo = oooo_blk.reshape(o_r, 2, o_c, row_n, o_r, 2, o_c).transpose(1, 0, 2, 3, 5, 4, 6)
        oooo = relative(oooo.reshape(rows, row_n, rows), r, 1).reshape(rows, row_n * rows)
        w_hole = (oooo.astype(f32) + 0.5 * x_full).astype(jnp.bfloat16)

        q_own = 2 * x + k
        tl = jnp.where(y == c, lax.dynamic_index_in_dim(g, q_own, 1, keepdims=False), tl_recv)
        base, brecv, drecv = ladder(
            tl.reshape(row_n * rows, piece), w_hole.T, vvvvv_blk, t_perm, vo_perm, im, d_blk)
        return finish(base, brecv, d_blk, drecv, r3.reshape(o_r * n_vir, o_c * n_vir), n_vir)

    return jax.shard_map(
        local_sweep,
        mesh=mesh,
        in_specs=(P("row", "col"), P("row", "col"), P("row", "col"), P("row", "col"), P("row", None), P(None, "col")),
        out_specs=P("row", "col"),
        check_vma=False,
    )
```
